256 devices in a mesh: ty: 32 (over y, z_lo, core), tx: 8 (over x, z_hi).
Axes of the slice: x: 4, y: 4, z: 8 (z_hi: 2, z_lo: 4; z = z_hi * 4 + z_lo), core: 2. Of those that a mesh axis runs over, the one named last changes fastest.
Arguments:
- ctrl: float32 [32, 8, 512, 640], P('ty', 'tx'), may hold values from -6 to 6
- interp_wt: float32 [32, 8, 4, 128, 384], P('ty', 'tx'), may hold values from -0.3125 to 0.3125
- interp_cols: int32 [32, 8, 4, 384], P('ty', 'tx'), may hold values from 0 to 1023
- conv_wt: float32 [32, 8, 4, 128, 512], P('ty', 'tx'), may hold values from -0.25 to 0.25
- conv_cols: int32 [32, 8, 4, 512], P('ty', 'tx'), may hold values from 0 to 1023
- halo_index: int32 [32, 8, 8, 64], P('ty', 'tx'), may hold values from 0 to 511
- valid: int32 [32, 8], P('ty', 'tx'), may hold values from 256 to 512
Outputs:
- localized: float32 [32, 8, 512, 640], P('ty', 'tx')
The draws below stay inside these ranges and needn't reach their ends.
Inputs may be any that keep to these rules, and one draw needn't show every extreme that they name: `interp_cols`: indices into a tile's extended subgrid of 1024 rows; repeats are allowed. `conv_cols`: indices into a tile's extended subgrid; repeats are allowed. `halo_index`: owned row indices; repeats are allowed.
All inputs are finite; a program needn't handle non-finite values.
Results may differ from the reference program's by a relative error of at most 0.0001.
Values sent between devices are 32-bit elements; how exact they have to be, the bound alone decides.
A program may use at most 64 MiB of HBM per device.

```python
import jax
import jax.numpy as jnp
from jax import lax

NODES = 512
GRID = 512
HALO = 64
GROWS = 128
GCOLS = 384
CROWS = 128
CCOLS = 512
FEAT = 640
EXT = 1024
GBLK = 4
CBLK = 4
N_TY = 32
N_TX = 8


def with_ends(array, key, smallest, top_value):
    longest = array.shape.index(max(array.shape))
    spots = []
    for shift in (0, 1):
        where = [jax.random.randint(jax.random.fold_in(key, axis), (), 0, length) for axis, length in enumerate(array.shape)]
        where[longest] = (where[longest] + shift) % array.shape[longest]
        spots.append(tuple(where))
    return array.at[spots[0]].set(smallest).at[spots[1]].set(top_value)


def steps_of(stream_key, dims, cuts, low, largest):
    gain, own = 1.0, jax.random.fold_in(stream_key, 6)
    for position, blocks in cuts:
        steps = jnp.exp(jax.random.uniform(jax.random.fold_in(own, position), (blocks,), jnp.float32, low / len(cuts), largest / len(cuts)))
        gain = gain * jnp.repeat(steps, dims[position] // blocks).reshape([-1 if axis == position else 1 for axis in range(len(dims))])
    return gain


def scatter_about(rng, shape, scale, most, cuts=(), kind=jnp.bfloat16):
    gain = steps_of(rng, shape, cuts, -0.22, 0.18) if cuts else 1.0
    values = jax.random.normal(rng, shape, jnp.float32) * scale * gain
    return jnp.minimum(jnp.maximum(values, -most), most).astype(kind)


def setup_inputs(seed: int = 0) -> dict:
    keys = jax.random.split(jax.random.key(seed), 8)
    return {
        "ctrl": scatter_about(keys[0], (N_TY, N_TX, GRID, FEAT), 1.0, 6.0, ((0, 32), (1, 8)), jnp.float32),
        "interp_wt": scatter_about(keys[1], (N_TY, N_TX, GBLK, GROWS, GCOLS), GCOLS ** -0.5, 0.3125, ((0, 32), (1, 8)), jnp.float32),
        "interp_cols": with_ends(jax.random.randint(keys[2], (N_TY, N_TX, GBLK, GCOLS), 0, EXT), jax.random.fold_in(keys[2], 1), 0, EXT - 1).astype(jnp.int32),
        "conv_wt": scatter_about(keys[3], (N_TY, N_TX, CBLK, CROWS, CCOLS), CCOLS ** -0.5, 0.25, ((0, 32), (1, 8)), jnp.float32),
        "conv_cols": with_ends(jax.random.randint(keys[4], (N_TY, N_TX, CBLK, CCOLS), 0, EXT), jax.random.fold_in(keys[4], 1), 0, EXT - 1).astype(jnp.int32),
        "halo_index": with_ends(jax.random.randint(keys[5], (N_TY, N_TX, 8, HALO), 0, NODES), jax.random.fold_in(keys[5], 1), 0, NODES - 1).astype(jnp.int32),
        "valid": with_ends(jax.random.randint(keys[6], (N_TY, N_TX), GRID // 2, GRID + 1), jax.random.fold_in(keys[6], 1), GRID // 2, GRID).astype(jnp.int32),
    }


DIRECTIONS = ((-1, -1), (-1, 0), (-1, 1), (0, -1), (0, 1), (1, -1), (1, 0), (1, 1))


def neighbour(tiles, row_off, col_off):
    shifted = jnp.roll(tiles, -col_off, axis=1)
    edge = jnp.zeros_like(shifted[:1])
    if row_off == 1:
        return jnp.concatenate([shifted[1:], edge], axis=0)
    if row_off == -1:
        return jnp.concatenate([edge, shifted[:-1]], axis=0)
    return shifted


def over_tiles(func, *arrays):
    rows_t, cols_t = arrays[0].shape[:2]
    flat = tuple(item.reshape((rows_t * cols_t,) + item.shape[2:]) for item in arrays)
    result = lax.map(lambda packed: func(*packed), flat)
    return result.reshape((rows_t, cols_t) + result.shape[1:])


def forward_blocks(weights, cols, source):
    gathered = jnp.take(source, cols, axis=0)
    result = jnp.einsum("bgc,bcf->bgf", weights, gathered, precision=lax.Precision.HIGHEST)
    return result.reshape(-1, source.shape[1])


def adjoint_blocks(weights, cols, values):
    blocks = values.reshape(weights.shape[0], weights.shape[1], values.shape[1])
    contrib = jnp.einsum("bgc,bgf->bcf", weights, blocks, precision=lax.Precision.HIGHEST)
    return jax.ops.segment_sum(contrib.reshape(-1, values.shape[1]), cols.reshape(-1), num_segments=EXT)


def accumulate(contrib, halo_index):
    owned = contrib[:, :, :NODES]
    slots = contrib[:, :, NODES:].reshape(contrib.shape[0], contrib.shape[1], 8, HALO, FEAT)
    for slot_id in range(8):
        row_off, col_off = DIRECTIONS[slot_id]
        arrived = neighbour(slots[:, :, slot_id], row_off, col_off)
        owned = owned + over_tiles(lambda vals, idx: jax.ops.segment_sum(vals, idx, num_segments=NODES), arrived, halo_index[:, :, slot_id])
    return owned


def extend(owned, halo_index):
    sends = over_tiles(lambda field, idx: jnp.take(field, idx, axis=0), owned, halo_index)
    slots = []
    for slot_id in range(8):
        row_off, col_off = DIRECTIONS[slot_id]
        slots.append(neighbour(sends[:, :, slot_id], -row_off, -col_off))
    stacked = jnp.stack(slots, axis=2).reshape(owned.shape[0], owned.shape[1], 8 * HALO, FEAT)
    return jnp.concatenate([owned, stacked], axis=2)


def reference(ctrl, interp_wt, interp_cols, conv_wt, conv_cols, halo_index, valid):
    positions = jnp.arange(GRID, dtype=jnp.int32)
    mask = (positions[None, None, :] < valid[:, :, None]).astype(jnp.float32)[..., None]
    masked = ctrl * mask
    a_ext = over_tiles(adjoint_blocks, interp_wt, interp_cols, masked)
    summed = accumulate(a_ext, halo_index)
    b_ext = over_tiles(adjoint_blocks, conv_wt, conv_cols, summed)
    spread = accumulate(b_ext, halo_index)
    smooth = over_tiles(forward_blocks, conv_wt, conv_cols, extend(spread, halo_index))
    result = over_tiles(forward_blocks, interp_wt, interp_cols, extend(smooth, halo_index))
    return result * mask
```

```python
import functools

import jax
import jax.numpy as jnp
from jax import lax
from jax.experimental import pallas as pl
from jax.experimental.pallas import tpu as pltpu
from jax.sharding import PartitionSpec as P

DIRECTIONS = ((-1, -1), (-1, 0), (-1, 1), (0, -1), (0, 1), (1, -1), (1, 0), (1, 1))
LANES = 128
MESH = pl.DeviceIdType.MESH
ADJOINT, FORWARD = -1, 1


def split(value):
    high = value.astype(jnp.bfloat16)
    low = (value - high.astype(jnp.float32)).astype(jnp.bfloat16)
    return high, low


def dot(left, right):
    return jnp.dot(left, right, preferred_element_type=jnp.float32)


def dot_rows(left, right):
    return lax.dot_general(
        left, right, (((1,), (1,)), ((), ())), preferred_element_type=jnp.float32
    )


def select(onehot, value):
    high, low = split(value)
    both = dot(onehot, jnp.concatenate([high, low], axis=1))
    return both[:, :LANES] + both[:, LANES:]


def product(high_ref, low_ref, value):
    high, low = split(value)
    both = dot(high_ref[...], jnp.concatenate([high, low], axis=1))
    return both[:, :LANES] + both[:, LANES:] + dot(low_ref[...], high)


def kernel(
    n_ty, n_tx, ctrl, iwt, icols, cwt, ccols, halo, valid, out,
    sends, recvs, owned, dense, dense_t, pick, spread, send_sem, recv_sem,
):
    row, col = lax.axis_index("ty"), lax.axis_index("tx")
    own_rows = pick.shape[1]
    slots = pick.shape[0]
    extent = own_rows + slots
    slot = slots // 8
    chunks = recvs.shape[1]
    grid_rows = ctrl.shape[0]

    def device(slot_id, sign):
        row_off, col_off = DIRECTIONS[slot_id]
        return (
            lax.rem(row + sign * row_off + n_ty, n_ty),
            lax.rem(col + sign * col_off + n_tx, n_tx),
        )

    barrier = pltpu.get_barrier_semaphore()
    for slot_id in range(8):
        pl.semaphore_signal(
            barrier, inc=1, device_id=device(slot_id, FORWARD), device_id_type=MESH
        )

    def densify_t(which, weights, cols):
        def step(block, _):
            ids = lax.broadcasted_iota(jnp.int32, (extent, weights.shape[2]), 0)
            onehot = jnp.where(ids == cols[block], 1.0, 0.0).astype(jnp.bfloat16)
            high, low = split(weights[block])
            lanes = pl.ds(pl.multiple_of(block * LANES, LANES), LANES)
            turned = dot_rows(onehot, high) + dot_rows(onehot, low)
            high, low = split(turned)
            dense_t[which, 0, :, lanes] = high
            dense_t[which, 1, :, lanes] = low
            return 0

        lax.fori_loop(0, weights.shape[0], step, 0)

    def densify(which, weights, cols):
        def step(block, _):
            ids = lax.broadcasted_iota(jnp.int32, (extent, weights.shape[2]), 0)
            onehot = jnp.where(ids == cols[block], 1.0, 0.0).astype(jnp.bfloat16)
            high, low = split(weights[block])
            rows = pl.ds(pl.multiple_of(block * LANES, LANES), LANES)
            plain = dot_rows(high, onehot) + dot_rows(low, onehot)
            high, low = split(plain)
            dense[which, 0, rows, :] = high
            dense[which, 1, rows, :] = low
            return 0

        lax.fori_loop(0, weights.shape[0], step, 0)

    def copy(stage, chunk, slot_id, sign):
        rows = pl.ds(slot_id * slot, slot)
        return pltpu.make_async_remote_copy(
            src_ref=sends.at[stage, chunk, rows],
            dst_ref=recvs.at[stage, chunk, rows],
            send_sem=send_sem.at[stage, chunk],
            recv_sem=recv_sem.at[stage, chunk],
            device_id=device(slot_id, sign),
            device_id_type=MESH,
        )

    def send(stage, chunk, sign):
        for slot_id in range(8):
            copy(stage, chunk, slot_id, sign).start()

    def whole(stage, chunk):
        return pltpu.make_async_remote_copy(
            src_ref=sends.at[stage, chunk],
            dst_ref=recvs.at[stage, chunk],
            send_sem=send_sem.at[stage, chunk],
            recv_sem=recv_sem.at[stage, chunk],
            device_id=device(0, FORWARD),
            device_id_type=MESH,
        )

    slot_rows = lax.broadcasted_iota(jnp.int32, (slots, LANES), 0)
    first, last = row == 0, row == n_ty - 1

    def arrived(stage, chunk, sign):
        whole(stage, chunk).wait_recv()
        top, bottom = (first, last) if sign == ADJOINT else (last, first)
        missing = ((slot_rows < 3 * slot) & top) | ((slot_rows >= 5 * slot) & bottom)
        return jnp.where(missing, 0.0, recvs[stage, chunk])

    grid_ids = lax.broadcasted_iota(jnp.int32, (grid_rows, LANES), 0)
    inside = grid_ids < valid[...]

    densify_t(0, iwt, icols)
    pl.semaphore_wait(barrier, 8)

    def lanes_of(chunk):
        return pl.ds(pl.multiple_of(chunk * LANES, LANES), LANES)

    def stage0(chunk, _):
        masked = jnp.where(inside, ctrl[:, lanes_of(chunk)], 0.0)
        ext = product(dense_t.at[0, 0], dense_t.at[0, 1], masked)
        owned[chunk] = ext[:own_rows]
        sends[0, chunk] = ext[own_rows:]
        send(0, chunk, ADJOINT)
        return 0

    lax.fori_loop(0, chunks, stage0, 0)

    ids = lax.broadcasted_iota(jnp.int32, (own_rows, slots), 0)
    hot = jnp.where(ids == halo[...], 1.0, 0.0)
    spread[...] = hot.astype(jnp.bfloat16)
    pick[...] = hot.T.astype(jnp.bfloat16)
    densify_t(1, cwt, ccols)
    densify(1, cwt, ccols)
    densify(0, iwt, icols)

    def stage1(chunk, _):
        total = owned[chunk] + select(spread[...], arrived(0, chunk, ADJOINT))
        ext = product(dense_t.at[1, 0], dense_t.at[1, 1], total)
        owned[chunk] = ext[:own_rows]
        sends[1, chunk] = ext[own_rows:]
        send(1, chunk, ADJOINT)
        return 0

    lax.fori_loop(0, chunks, stage1, 0)

    def stage2(chunk, _):
        total = owned[chunk] + select(spread[...], arrived(1, chunk, ADJOINT))
        owned[chunk] = total
        sends[2, chunk] = select(pick[...], total)
        send(2, chunk, FORWARD)
        return 0

    lax.fori_loop(0, chunks, stage2, 0)

    def stage3(chunk, _):
        ext = jnp.concatenate([owned[chunk], arrived(2, chunk, FORWARD)], axis=0)
        smooth = product(dense.at[1, 0], dense.at[1, 1], ext)
        owned[chunk] = smooth
        sends[3, chunk] = select(pick[...], smooth)
        send(3, chunk, FORWARD)
        return 0

    lax.fori_loop(0, chunks, stage3, 0)

    def stage4(chunk, _):
        ext = jnp.concatenate([owned[chunk], arrived(3, chunk, FORWARD)], axis=0)
        result = product(dense.at[0, 0], dense.at[0, 1], ext)
        out[:, lanes_of(chunk)] = jnp.where(inside, result, 0.0)
        return 0

    lax.fori_loop(0, chunks, stage4, 0)

    def drain(chunk, _):
        for stage in range(4):
            whole(stage, chunk).wait_send()
        return 0

    lax.fori_loop(0, chunks, drain, 0)


def body(n_ty, n_tx, ctrl, interp_wt, interp_cols, conv_wt, conv_cols, halo_index, valid):
    field = ctrl[0, 0]
    iwt, cwt = interp_wt[0, 0], conv_wt[0, 0]
    grid_rows, width = field.shape
    own_rows = cwt.shape[0] * cwt.shape[1]
    slots = halo_index.shape[2] * halo_index.shape[3]
    extent = own_rows + slots
    chunks = width // LANES
    vmem = pl.BlockSpec(memory_space=pltpu.VMEM)
    f32, bf16 = jnp.float32, jnp.bfloat16
    result = pl.pallas_call(
        functools.partial(kernel, n_ty, n_tx),
        out_shape=jax.ShapeDtypeStruct((grid_rows, width), f32),
        in_specs=[vmem] * 7,
        out_specs=vmem,
        scratch_shapes=[
            pltpu.VMEM((4, chunks, slots, LANES), f32),
            pltpu.VMEM((4, chunks, slots, LANES), f32),
            pltpu.VMEM((chunks, own_rows, LANES), f32),
            pltpu.VMEM((2, 2, own_rows, extent), bf16),
            pltpu.VMEM((2, 2, extent, own_rows), bf16),
            pltpu.VMEM((slots, own_rows), bf16),
            pltpu.VMEM((own_rows, slots), bf16),
            pltpu.SemaphoreType.DMA((4, chunks)),
            pltpu.SemaphoreType.DMA((4, chunks)),
        ],
        compiler_params=pltpu.CompilerParams(collective_id=0, has_side_effects=True),
    )(
        field,
        iwt,
        interp_cols[0, 0][:, None, :],
        cwt,
        conv_cols[0, 0][:, None, :],
        halo_index.reshape(1, slots),
        jnp.broadcast_to(valid.reshape(1, 1), (1, LANES)),
    )
    return result[None, None]


def solution(mesh):
    placed = (
        P("ty", "tx", None, None),
        P("ty", "tx", None, None, None),
        P("ty", "tx", None, None),
        P("ty", "tx", None, None, None),
        P("ty", "tx", None, None),
        P("ty", "tx", None, None),
        P("ty", "tx"),
    )
    return jax.shard_map(
        functools.partial(body, mesh.shape["ty"], mesh.shape["tx"]),
        mesh=mesh,
        in_specs=placed,
        out_specs=P("ty", "tx", None, None),
        check_vma=False,
    )
```

```python
import functools

import jax
import jax.numpy as jnp
from jax import lax
from jax.experimental import pallas as pl
from jax.experimental.pallas import tpu as pltpu
from jax.sharding import PartitionSpec as P

DIRECTIONS = ((-1, -1), (-1, 0), (-1, 1), (0, -1), (0, 1), (1, -1), (1, 0), (1, 1))
LANES = 128
MESH = pl.DeviceIdType.MESH
ADJOINT, FORWARD = -1, 1


def split(value):
    high = value.astype(jnp.bfloat16)
    low = (value - high.astype(jnp.float32)).astype(jnp.bfloat16)
    return high, low


def dot(left, right):
    return jnp.dot(left, right, preferred_element_type=jnp.float32)


def dot_rows(left, right):
    return lax.dot_general(
        left, right, (((1,), (1,)), ((), ())), preferred_element_type=jnp.float32
    )


def select(onehot, value):
    high, low = split(value)
    both = dot(onehot, jnp.concatenate([high, low], axis=1))
    return both[:, :LANES] + both[:, LANES:]


def product(high_ref, low_ref, value):
    high, low = split(value)
    both = dot(high_ref[...], jnp.concatenate([high, low], axis=1))
    return both[:, :LANES] + both[:, LANES:] + dot(low_ref[...], high)


def host_of(row, col):
    band, pair, lower = row // 8, (row % 8) // 2, row % 2
    ring = band + (band // 2) * (3 - 2 * band)
    placed = ring + ((lower + pair) % 2) * (3 - 2 * ring)
    level = pair + ring * (3 - 2 * pair)
    return 8 * placed + 2 * level + col % 2, 2 * (col // 2) + band // 2


def tile_of(ty, tx):
    placed, level = ty // 8, (ty % 8) // 2
    ring = placed + (placed // 2) * (3 - 2 * placed)
    pair = level + ring * (3 - 2 * level)
    band = ring + (tx % 2) * (3 - 2 * ring)
    lower = (placed // 2 + pair) % 2
    return 8 * band + 2 * pair + lower, 2 * (tx // 2) + ty % 2


def across(ty, tx):
    return 8 * (3 - ty // 8) + ty % 8, tx


def steps_of(ty, tx):
    to_ty, to_tx = host_of(ty, tx)
    turns = to_ty // 8 != ty // 8
    climbs = ((to_ty % 8) // 2 != (ty % 8) // 2) | (to_tx % 2 != tx % 2)
    return turns & climbs


def kernel(
    n_ty, n_tx, ctrl, iwt, cwt, ints, out,
    field, iw, cw, ids, relay_field, relay_iw, relay_cw, relay_ids,
    sends, recvs, owned, dense, dense_t, pick, spread, results,
    first_sem, home_sem, relay_sem, pass_sem, send_sem, recv_sem, back_sem, done_sem,
):
    ty, tx = lax.axis_index("ty"), lax.axis_index("tx")
    own_rows = pick.shape[1]
    slots = pick.shape[0]
    extent = own_rows + slots
    slot = slots // 8
    chunks = recvs.shape[1]
    grid_rows = ctrl.shape[0]
    blocks = iw.shape[0]

    row, col = tile_of(ty, tx)
    host = host_of(ty, tx)
    partner = across(ty, tx)
    relayed = host_of(*partner)
    feeder = across(row, col)

    stays = (host[0] == ty) & (host[1] == tx)
    by_relay = steps_of(ty, tx)
    direct = jnp.logical_not(stays | by_relay)
    relays = steps_of(*partner)

    def device(slot_id, sign):
        row_off, col_off = DIRECTIONS[slot_id]
        return host_of(
            (row + sign * row_off + n_ty) % n_ty, (col + sign * col_off + n_tx) % n_tx
        )

    barrier = pltpu.get_barrier_semaphore()
    greeted = [device(slot_id, FORWARD) for slot_id in range(8)]
    greeted += [host, (row, col), partner, feeder]
    for other in greeted:
        pl.semaphore_signal(barrier, inc=1, device_id=other, device_id_type=MESH)
    pl.semaphore_wait(barrier, len(greeted))

    def lanes_of(chunk):
        return pl.ds(chunk * LANES, LANES)

    mine = [ints] + [iwt.at[b] for b in range(blocks)] + [cwt.at[b] for b in range(blocks)]
    mine += [ctrl.at[:, lanes_of(c)] for c in range(chunks)]
    final = [ids] + [iw.at[b] for b in range(blocks)] + [cw.at[b] for b in range(blocks)]
    final += [field.at[c] for c in range(chunks)]
    passing = [relay_ids] + [relay_iw.at[b] for b in range(blocks)]
    passing += [relay_cw.at[b] for b in range(blocks)]
    passing += [relay_field.at[c] for c in range(chunks)]
    items = len(mine)

    def to_host(item):
        return pltpu.make_async_remote_copy(
            src_ref=mine[item], dst_ref=final[item],
            send_sem=first_sem.at[item], recv_sem=home_sem.at[item],
            device_id=host, device_id_type=MESH,
        )

    def to_relay(item):
        return pltpu.make_async_remote_copy(
            src_ref=mine[item], dst_ref=passing[item],
            send_sem=first_sem.at[item], recv_sem=relay_sem.at[item],
            device_id=partner, device_id_type=MESH,
        )

    def pass_on(item):
        return pltpu.make_async_remote_copy(
            src_ref=passing[item], dst_ref=final[item],
            send_sem=pass_sem.at[item], recv_sem=home_sem.at[item],
            device_id=relayed, device_id_type=MESH,
        )

    @pl.when(by_relay)
    def _():
        for item in range(items):
            to_relay(item).start()

    @pl.when(direct)
    def _():
        for item in range(items):
            to_host(item).start()

    @pl.when(stays)
    def _():
        for item in range(items):
            pltpu.make_async_copy(mine[item], final[item], home_sem.at[item]).start()

    @pl.when(relays)
    def _():
        for item in range(items):
            to_relay(item).wait_recv()
            pass_on(item).start()

    def landed(item):
        to_host(item).wait_recv()

    def onehot_of(base, count):
        pieces = []
        for piece in range(count):
            rows = lax.broadcasted_iota(jnp.int32, (extent, LANES), 0)
            same = rows == ids[pl.ds(base + piece, 1), :]
            pieces.append(jnp.where(same, 1.0, 0.0).astype(jnp.bfloat16))
        return jnp.concatenate(pieces, axis=1)

    def densify(which, weights, base):
        count = weights.shape[2] // LANES

        def step(block, _):
            onehot = onehot_of(base + block * count, count)
            high, low = split(weights[block])
            lanes = pl.ds(pl.multiple_of(block * LANES, LANES), LANES)
            turned = dot_rows(onehot, high) + dot_rows(onehot, low)
            plain = dot_rows(high, onehot) + dot_rows(low, onehot)
            high, low = split(turned)
            dense_t[which, 0, :, lanes] = high
            dense_t[which, 1, :, lanes] = low
            high, low = split(plain)
            dense[which, 0, lanes, :] = high
            dense[which, 1, lanes, :] = low
            return 0

        lax.fori_loop(0, blocks, step, 0)

    def copy(stage, chunk, slot_id, sign):
        rows = pl.ds(slot_id * slot, slot)
        return pltpu.make_async_remote_copy(
            src_ref=sends.at[stage, chunk, rows],
            dst_ref=recvs.at[stage, chunk, rows],
            send_sem=send_sem.at[stage, chunk],
            recv_sem=recv_sem.at[stage, chunk],
            device_id=device(slot_id, sign),
            device_id_type=MESH,
        )

    def send(stage, chunk, sign):
        for slot_id in range(8):
            copy(stage, chunk, slot_id, sign).start()

    def whole(stage, chunk):
        return pltpu.make_async_remote_copy(
            src_ref=sends.at[stage, chunk],
            dst_ref=recvs.at[stage, chunk],
            send_sem=send_sem.at[stage, chunk],
            recv_sem=recv_sem.at[stage, chunk],
            device_id=device(0, FORWARD),
            device_id_type=MESH,
        )

    slot_rows = lax.broadcasted_iota(jnp.int32, (slots, LANES), 0)
    first, last = row == 0, row == n_ty - 1

    def arrived(stage, chunk, sign):
        whole(stage, chunk).wait_recv()
        top, bottom = (first, last) if sign == ADJOINT else (last, first)
        missing = ((slot_rows < 3 * slot) & top) | ((slot_rows >= 5 * slot) & bottom)
        return jnp.where(missing, 0.0, recvs[stage, chunk])

    icount, ccount = iw.shape[2] // LANES, cw.shape[2] // LANES
    halo_base = blocks * (icount + ccount)
    valid_base = halo_base + slots // LANES

    for item in range(1 + blocks):
        landed(item)
    grid_ids = lax.broadcasted_iota(jnp.int32, (grid_rows, LANES), 0)

    def inside():
        return grid_ids < ids[pl.ds(valid_base, 1), :]

    densify(0, iw, 0)
    for piece in range(slots // LANES):
        rows = lax.broadcasted_iota(jnp.int32, (own_rows, LANES), 0)
        same = rows == ids[pl.ds(halo_base + piece, 1), :]
        hot = jnp.where(same, 1.0, 0.0)
        lanes = pl.ds(piece * LANES, LANES)
        spread[:, lanes] = hot.astype(jnp.bfloat16)
        pick[lanes, :] = hot.T.astype(jnp.bfloat16)
    for item in range(1 + blocks, 1 + 2 * blocks):
        landed(item)
    densify(1, cw, blocks * icount)

    def field_landed(chunk):
        pltpu.make_async_remote_copy(
            src_ref=results.at[chunk], dst_ref=field.at[chunk],
            send_sem=first_sem.at[1 + 2 * blocks + chunk],
            recv_sem=home_sem.at[1 + 2 * blocks + chunk],
            device_id=host, device_id_type=MESH,
        ).wait_recv()

    def stage0(chunk):
        field_landed(chunk)
        masked = jnp.where(inside(), field[chunk], 0.0)
        ext = product(dense_t.at[0, 0], dense_t.at[0, 1], masked)
        owned[chunk] = ext[:own_rows]
        sends[0, chunk] = ext[own_rows:]
        send(0, chunk, ADJOINT)

    def stage1(chunk):
        total = owned[chunk] + select(spread[...], arrived(0, chunk, ADJOINT))
        ext = product(dense_t.at[1, 0], dense_t.at[1, 1], total)
        owned[chunk] = ext[:own_rows]
        sends[1, chunk] = ext[own_rows:]
        send(1, chunk, ADJOINT)

    def stage2(chunk):
        total = owned[chunk] + select(spread[...], arrived(1, chunk, ADJOINT))
        owned[chunk] = total
        sends[2, chunk] = select(pick[...], total)
        send(2, chunk, FORWARD)

    def stage3(chunk):
        ext = jnp.concatenate([owned[chunk], arrived(2, chunk, FORWARD)], axis=0)
        smooth = product(dense.at[1, 0], dense.at[1, 1], ext)
        owned[chunk] = smooth
        sends[3, chunk] = select(pick[...], smooth)
        send(3, chunk, FORWARD)

    def back(chunk):
        lanes = pl.ds(pl.multiple_of(chunk * LANES, LANES), LANES)
        return pltpu.make_async_remote_copy(
            src_ref=results.at[chunk], dst_ref=out.at[:, lanes],
            send_sem=back_sem.at[chunk], recv_sem=done_sem.at[chunk],
            device_id=(row, col), device_id_type=MESH,
        )

    def stage4(chunk):
        ext = jnp.concatenate([owned[chunk], arrived(3, chunk, FORWARD)], axis=0)
        result = product(dense.at[0, 0], dense.at[0, 1], ext)
        results[chunk] = jnp.where(inside(), result, 0.0)

        @pl.when(stays)
        def _():
            lanes = pl.ds(pl.multiple_of(chunk * LANES, LANES), LANES)
            pltpu.make_async_copy(results.at[chunk], out.at[:, lanes], done_sem.at[chunk]).start()

        @pl.when(jnp.logical_not(stays))
        def _():
            back(chunk).start()

    stages = (stage0, stage1, stage2, stage3, stage4)

    def wave(step, _):
        for number, stage in enumerate(stages):
            chunk = step - number

            @pl.when((chunk >= 0) & (chunk < chunks))
            def _():
                stage(chunk)

        return 0

    lax.fori_loop(0, chunks + len(stages) - 1, wave, 0)

    @pl.when(by_relay | direct)
    def _():
        for item in range(items):
            to_host(item).wait_send()

    @pl.when(relays)
    def _():
        for item in range(items):
            pass_on(item).wait_send()

    @pl.when(jnp.logical_not(stays))
    def _():
        for chunk in range(chunks):
            back(chunk).wait_send()

    for chunk in range(chunks):
        for stage in range(4):
            whole(stage, chunk).wait_send()
        back(chunk).wait_recv()


def body(n_ty, n_tx, ctrl, interp_wt, interp_cols, conv_wt, conv_cols, halo_index, valid):
    field = ctrl[0, 0]
    iwt, cwt = interp_wt[0, 0], conv_wt[0, 0]
    grid_rows, width = field.shape
    blocks = iwt.shape[0]
    own_rows = blocks * cwt.shape[1]
    slots = halo_index.shape[2] * halo_index.shape[3]
    extent = own_rows + slots
    chunks = width // LANES
    ints = jnp.concatenate(
        [
            interp_cols.reshape(-1, LANES),
            conv_cols.reshape(-1, LANES),
            halo_index.reshape(-1, LANES),
            jnp.broadcast_to(valid.reshape(1, 1), (8, LANES)),
        ]
    )
    vmem = pl.BlockSpec(memory_space=pltpu.VMEM)
    f32, bf16 = jnp.float32, jnp.bfloat16
    tile = [
        pltpu.VMEM((chunks, grid_rows, LANES), f32),
        pltpu.VMEM(iwt.shape, f32),
        pltpu.VMEM(cwt.shape, f32),
        pltpu.VMEM(ints.shape, jnp.int32),
    ]
    items = 1 + 2 * blocks + chunks
    dma = pltpu.SemaphoreType.DMA
    result = pl.pallas_call(
        functools.partial(kernel, n_ty, n_tx),
        out_shape=jax.ShapeDtypeStruct((grid_rows, width), f32),
        in_specs=[vmem] * 4,
        out_specs=vmem,
        scratch_shapes=tile
        + tile
        + [
            pltpu.VMEM((4, chunks, slots, LANES), f32),
            pltpu.VMEM((4, chunks, slots, LANES), f32),
            pltpu.VMEM((chunks, own_rows, LANES), f32),
            pltpu.VMEM((2, 2, own_rows, extent), bf16),
            pltpu.VMEM((2, 2, extent, own_rows), bf16),
            pltpu.VMEM((slots, own_rows), bf16),
            pltpu.VMEM((own_rows, slots), bf16),
            pltpu.VMEM((chunks, grid_rows, LANES), f32),
            dma((items,)),
            dma((items,)),
            dma((items,)),
            dma((items,)),
            dma((4, chunks)),
            dma((4, chunks)),
            dma((chunks,)),
            dma((chunks,)),
        ],
        compiler_params=pltpu.CompilerParams(collective_id=0, has_side_effects=True),
    )(field, iwt, cwt, ints)
    return result[None, None]


def solution(mesh):
    placed = (
        P("ty", "tx", None, None),
        P("ty", "tx", None, None, None),
        P("ty", "tx", None, None),
        P("ty", "tx", None, None, None),
        P("ty", "tx", None, None),
        P("ty", "tx", None, None),
        P("ty", "tx"),
    )
    return jax.shard_map(
        functools.partial(body, mesh.shape["ty"], mesh.shape["tx"]),
        mesh=mesh,
        in_specs=placed,
        out_specs=P("ty", "tx", None, None),
        check_vma=False,
    )
```

```python
import functools

import jax
import jax.numpy as jnp
from jax import lax
from jax.experimental import pallas as pl
from jax.experimental.pallas import tpu as pltpu
from jax.sharding import PartitionSpec as P

DIRECTIONS = ((-1, -1), (-1, 0), (-1, 1), (0, -1), (0, 1), (1, -1), (1, 0), (1, 1))
LANES = 128
MESH = pl.DeviceIdType.MESH
ADJOINT, FORWARD = -1, 1


def split(value):
    high = value.astype(jnp.bfloat16)
    low = (value - high.astype(jnp.float32)).astype(jnp.bfloat16)
    return high, low


def dot(left, right):
    return jnp.dot(left, right, preferred_element_type=jnp.float32)


def dot_rows(left, right):
    return lax.dot_general(
        left, right, (((1,), (1,)), ((), ())), preferred_element_type=jnp.float32
    )


def select(onehot, value):
    high, low = split(value)
    both = dot(onehot, jnp.concatenate([high, low], axis=1))
    return both[:, :LANES] + both[:, LANES:]


def product(high_ref, low_ref, value):
    high, low = split(value)
    both = dot(high_ref[...], jnp.concatenate([high, low], axis=1))
    return both[:, :LANES] + both[:, LANES:] + dot(low_ref[...], high)


def host_of(row, col):
    band, pair, lower = row // 8, (row % 8) // 2, row % 2
    ring = band + (band // 2) * (3 - 2 * band)
    placed = ring + ((lower + pair) % 2) * (3 - 2 * ring)
    level = pair + ring * (3 - 2 * pair)
    return 8 * placed + 2 * level + col % 2, 2 * (col // 2) + band // 2


def tile_of(ty, tx):
    placed, level = ty // 8, (ty % 8) // 2
    ring = placed + (placed // 2) * (3 - 2 * placed)
    pair = level + ring * (3 - 2 * level)
    band = ring + (tx % 2) * (3 - 2 * ring)
    lower = (placed // 2 + pair) % 2
    return 8 * band + 2 * pair + lower, 2 * (tx // 2) + ty % 2


def across(ty, tx):
    return 8 * (3 - ty // 8) + ty % 8, tx


def steps_of(ty, tx):
    to_ty, to_tx = host_of(ty, tx)
    turns = to_ty // 8 != ty // 8
    climbs = ((to_ty % 8) // 2 != (ty % 8) // 2) | (to_tx % 2 != tx % 2)
    return turns & climbs


def kernel(
    n_ty, n_tx, ctrl, iwt, cwt, icols, ccols, marks, out,
    field, iw, cw, ic, cc, mk, relay_field, relay_iw, relay_cw, relay_ic, relay_cc, relay_mk,
    sends, recvs, owned, dense, dense_t, pick, spread, results,
    first_sem, home_sem, relay_sem, pass_sem, send_sem, recv_sem, back_sem, done_sem,
):
    ty, tx = lax.axis_index("ty"), lax.axis_index("tx")
    own_rows = pick.shape[1]
    slots = pick.shape[0]
    extent = own_rows + slots
    slot = slots // 8
    chunks = recvs.shape[1]
    grid_rows = ctrl.shape[0]
    blocks = iw.shape[0]

    row, col = tile_of(ty, tx)
    host = host_of(ty, tx)
    partner = across(ty, tx)
    relayed = host_of(*partner)
    feeder = across(row, col)

    stays = (host[0] == ty) & (host[1] == tx)
    by_relay = steps_of(ty, tx)
    direct = jnp.logical_not(stays | by_relay)
    relays = steps_of(*partner)

    def device(slot_id, sign):
        row_off, col_off = DIRECTIONS[slot_id]
        return host_of(
            (row + sign * row_off + n_ty) % n_ty, (col + sign * col_off + n_tx) % n_tx
        )

    barrier = pltpu.get_barrier_semaphore()
    greeted = [device(slot_id, FORWARD) for slot_id in range(8)]
    greeted += [host, (row, col), partner, feeder]
    for other in greeted:
        pl.semaphore_signal(barrier, inc=1, device_id=other, device_id_type=MESH)
    pl.semaphore_wait(barrier, len(greeted))

    def lanes_of(chunk):
        return pl.ds(chunk * LANES, LANES)

    mine = [icols, ccols, marks] + [iwt.at[b] for b in range(blocks)] + [cwt.at[b] for b in range(blocks)]
    mine += [ctrl.at[:, lanes_of(c)] for c in range(chunks)]
    final = [ic, cc, mk] + [iw.at[b] for b in range(blocks)] + [cw.at[b] for b in range(blocks)]
    final += [field.at[c] for c in range(chunks)]
    passing = [relay_ic, relay_cc, relay_mk] + [relay_iw.at[b] for b in range(blocks)]
    passing += [relay_cw.at[b] for b in range(blocks)]
    passing += [relay_field.at[c] for c in range(chunks)]
    items = len(mine)

    def to_host(item):
        return pltpu.make_async_remote_copy(
            src_ref=mine[item], dst_ref=final[item],
            send_sem=first_sem.at[item], recv_sem=home_sem.at[item],
            device_id=host, device_id_type=MESH,
        )

    def to_relay(item):
        return pltpu.make_async_remote_copy(
            src_ref=mine[item], dst_ref=passing[item],
            send_sem=first_sem.at[item], recv_sem=relay_sem.at[item],
            device_id=partner, device_id_type=MESH,
        )

    def pass_on(item):
        return pltpu.make_async_remote_copy(
            src_ref=passing[item], dst_ref=final[item],
            send_sem=pass_sem.at[item], recv_sem=home_sem.at[item],
            device_id=relayed, device_id_type=MESH,
        )

    @pl.when(by_relay)
    def _():
        for item in range(items):
            to_relay(item).start()

    @pl.when(direct)
    def _():
        for item in range(items):
            to_host(item).start()

    @pl.when(stays)
    def _():
        for item in range(items):
            pltpu.make_async_copy(mine[item], final[item], home_sem.at[item]).start()

    @pl.when(relays)
    def _():
        for item in range(items):
            to_relay(item).wait_recv()
            pass_on(item).start()

    def landed(item):
        to_host(item).wait_recv()

    def densify(which, weights, cols):
        def step(block, _):
            rows = lax.broadcasted_iota(jnp.int32, (extent, weights.shape[2]), 0)
            onehot = jnp.where(rows == cols[pl.ds(block, 1), :], 1.0, 0.0).astype(jnp.bfloat16)
            high, low = split(weights[block])
            lanes = pl.ds(pl.multiple_of(block * LANES, LANES), LANES)
            turned = dot_rows(onehot, high) + dot_rows(onehot, low)
            plain = dot_rows(high, onehot) + dot_rows(low, onehot)
            high, low = split(turned)
            dense_t[which, 0, :, lanes] = high
            dense_t[which, 1, :, lanes] = low
            high, low = split(plain)
            dense[which, 0, lanes, :] = high
            dense[which, 1, lanes, :] = low
            return 0

        lax.fori_loop(0, blocks, step, 0)

    def copy(stage, chunk, slot_id, sign):
        rows = pl.ds(slot_id * slot, slot)
        return pltpu.make_async_remote_copy(
            src_ref=sends.at[stage, chunk, rows],
            dst_ref=recvs.at[stage, chunk, rows],
            send_sem=send_sem.at[stage, chunk],
            recv_sem=recv_sem.at[stage, chunk],
            device_id=device(slot_id, sign),
            device_id_type=MESH,
        )

    def send(stage, chunk, sign):
        for slot_id in (1, 6, 0, 2, 5, 7, 3, 4):
            copy(stage, chunk, slot_id, sign).start()

    def whole(stage, chunk):
        return pltpu.make_async_remote_copy(
            src_ref=sends.at[stage, chunk],
            dst_ref=recvs.at[stage, chunk],
            send_sem=send_sem.at[stage, chunk],
            recv_sem=recv_sem.at[stage, chunk],
            device_id=device(0, FORWARD),
            device_id_type=MESH,
        )

    slot_rows = lax.broadcasted_iota(jnp.int32, (slots, LANES), 0)
    first, last = row == 0, row == n_ty - 1

    def arrived(stage, chunk, sign):
        whole(stage, chunk).wait_recv()
        top, bottom = (first, last) if sign == ADJOINT else (last, first)
        missing = ((slot_rows < 3 * slot) & top) | ((slot_rows >= 5 * slot) & bottom)
        return jnp.where(missing, 0.0, recvs[stage, chunk])

    heads = items - 2 * blocks - chunks
    for item in range(heads + blocks):
        landed(item)
    grid_ids = lax.broadcasted_iota(jnp.int32, (grid_rows, LANES), 0)

    def inside():
        return grid_ids < mk[0:1, slot : slot + 1]

    densify(0, iw, ic)
    rows = lax.broadcasted_iota(jnp.int32, (own_rows, slot), 0)
    for piece in range(slots // LANES):
        pair = [mk[pl.ds(2 * piece + k, 1), 0:slot] for k in range(2)]
        hot = jnp.concatenate([jnp.where(rows == k, 1.0, 0.0) for k in pair], axis=1)
        lanes = pl.ds(piece * LANES, LANES)
        spread[:, lanes] = hot.astype(jnp.bfloat16)
        pick[lanes, :] = hot.T.astype(jnp.bfloat16)
    for item in range(heads + blocks, heads + 2 * blocks):
        landed(item)
    densify(1, cw, cc)

    def field_landed(chunk):
        pltpu.make_async_remote_copy(
            src_ref=results.at[chunk], dst_ref=field.at[chunk],
            send_sem=first_sem.at[heads + 2 * blocks + chunk],
            recv_sem=home_sem.at[heads + 2 * blocks + chunk],
            device_id=host, device_id_type=MESH,
        ).wait_recv()

    def stage0(chunk):
        field_landed(chunk)
        masked = jnp.where(inside(), field[chunk], 0.0)
        ext = product(dense_t.at[0, 0], dense_t.at[0, 1], masked)
        owned[chunk] = ext[:own_rows]
        sends[0, chunk] = ext[own_rows:]
        send(0, chunk, ADJOINT)

    def stage1(chunk):
        total = owned[chunk] + select(spread[...], arrived(0, chunk, ADJOINT))
        ext = product(dense_t.at[1, 0], dense_t.at[1, 1], total)
        owned[chunk] = ext[:own_rows]
        sends[1, chunk] = ext[own_rows:]
        send(1, chunk, ADJOINT)

    def stage2(chunk):
        total = owned[chunk] + select(spread[...], arrived(1, chunk, ADJOINT))
        owned[chunk] = total
        sends[2, chunk] = select(pick[...], total)
        send(2, chunk, FORWARD)

    def stage3(chunk):
        ext = jnp.concatenate([owned[chunk], arrived(2, chunk, FORWARD)], axis=0)
        smooth = product(dense.at[1, 0], dense.at[1, 1], ext)
        owned[chunk] = smooth
        sends[3, chunk] = select(pick[...], smooth)
        send(3, chunk, FORWARD)

    def back(chunk):
        lanes = pl.ds(pl.multiple_of(chunk * LANES, LANES), LANES)
        return pltpu.make_async_remote_copy(
            src_ref=results.at[chunk], dst_ref=out.at[:, lanes],
            send_sem=back_sem.at[chunk], recv_sem=done_sem.at[chunk],
            device_id=(row, col), device_id_type=MESH,
        )

    def stage4(chunk):
        ext = jnp.concatenate([owned[chunk], arrived(3, chunk, FORWARD)], axis=0)
        result = product(dense.at[0, 0], dense.at[0, 1], ext)
        results[chunk] = jnp.where(inside(), result, 0.0)

        @pl.when(stays)
        def _():
            lanes = pl.ds(pl.multiple_of(chunk * LANES, LANES), LANES)
            pltpu.make_async_copy(results.at[chunk], out.at[:, lanes], done_sem.at[chunk]).start()

        @pl.when(jnp.logical_not(stays))
        def _():
            back(chunk).start()

    stages = (stage0, stage1, stage2, stage3, stage4)

    def run(stage):
        def one(chunk, _):
            stage(chunk)
            return 0

        lax.fori_loop(0, chunks, one, 0)

    for stage in stages:
        run(stage)

    @pl.when(by_relay | direct)
    def _():
        for item in range(items):
            to_host(item).wait_send()

    @pl.when(relays)
    def _():
        for item in range(items):
            pass_on(item).wait_send()

    @pl.when(jnp.logical_not(stays))
    def _():
        for chunk in range(chunks):
            back(chunk).wait_send()

    for chunk in range(chunks):
        for stage in range(4):
            whole(stage, chunk).wait_send()
        back(chunk).wait_recv()


def body(n_ty, n_tx, ctrl, interp_wt, interp_cols, conv_wt, conv_cols, halo_index, valid):
    field = ctrl[0, 0]
    iwt, cwt = interp_wt[0, 0], conv_wt[0, 0]
    grid_rows, width = field.shape
    blocks = iwt.shape[0]
    own_rows = blocks * cwt.shape[1]
    slots = halo_index.shape[2] * halo_index.shape[3]
    extent = own_rows + slots
    chunks = width // LANES
    halo = halo_index[0, 0]
    marks = jnp.concatenate([halo, jnp.broadcast_to(valid, halo.shape)], axis=1)
    icols, ccols = interp_cols[0, 0], conv_cols[0, 0]
    hbm = pl.BlockSpec(memory_space=pl.ANY)
    f32, bf16 = jnp.float32, jnp.bfloat16
    tile = [
        pltpu.VMEM((chunks, grid_rows, LANES), f32),
        pltpu.VMEM(iwt.shape, f32),
        pltpu.VMEM(cwt.shape, f32),
        pltpu.VMEM(icols.shape, jnp.int32),
        pltpu.VMEM(ccols.shape, jnp.int32),
        pltpu.VMEM(marks.shape, jnp.int32),
    ]
    items = 3 + 2 * blocks + chunks
    dma = pltpu.SemaphoreType.DMA
    result = pl.pallas_call(
        functools.partial(kernel, n_ty, n_tx),
        out_shape=jax.ShapeDtypeStruct((grid_rows, width), f32),
        in_specs=[hbm] * 6,
        out_specs=hbm,
        scratch_shapes=tile
        + tile
        + [
            pltpu.VMEM((4, chunks, slots, LANES), f32),
            pltpu.VMEM((4, chunks, slots, LANES), f32),
            pltpu.VMEM((chunks, own_rows, LANES), f32),
            pltpu.VMEM((2, 2, own_rows, extent), bf16),
            pltpu.VMEM((2, 2, extent, own_rows), bf16),
            pltpu.VMEM((slots, own_rows), bf16),
            pltpu.VMEM((own_rows, slots), bf16),
            pltpu.VMEM((chunks, grid_rows, LANES), f32),
            dma((items,)),
            dma((items,)),
            dma((items,)),
            dma((items,)),
            dma((4, chunks)),
            dma((4, chunks)),
            dma((chunks,)),
            dma((chunks,)),
        ],
        compiler_params=pltpu.CompilerParams(collective_id=0, has_side_effects=True),
    )(field, iwt, cwt, icols, ccols, marks)
    return result[None, None]


def solution(mesh):
    placed = (
        P("ty", "tx", None, None),
        P("ty", "tx", None, None, None),
        P("ty", "tx", None, None),
        P("ty", "tx", None, None, None),
        P("ty", "tx", None, None),
        P("ty", "tx", None, None),
        P("ty", "tx"),
    )
    return jax.shard_map(
        functools.partial(body, mesh.shape["ty"], mesh.shape["tx"]),
        mesh=mesh,
        in_specs=placed,
        out_specs=P("ty", "tx", None, None),
        check_vma=False,
    )
```

```python
import functools

import jax
import jax.numpy as jnp
from jax import lax
from jax.experimental import pallas as pl
from jax.experimental.pallas import tpu as pltpu
from jax.sharding import PartitionSpec as P

DIRECTIONS = ((-1, -1), (-1, 0), (-1, 1), (0, -1), (0, 1), (1, -1), (1, 0), (1, 1))
LANES = 128
MESH = pl.DeviceIdType.MESH
ADJOINT, FORWARD = -1, 1


def split(value):
    high = value.astype(jnp.bfloat16)
    low = (value - high.astype(jnp.float32)).astype(jnp.bfloat16)
    return high, low


def dot(left, right):
    return jnp.dot(left, right, preferred_element_type=jnp.float32)


def dot_rows(left, right):
    return lax.dot_general(
        left, right, (((1,), (1,)), ((), ())), preferred_element_type=jnp.float32
    )


def select(onehot, value):
    high, low = split(value)
    both = dot(onehot, jnp.concatenate([high, low], axis=1))
    return both[:, :LANES] + both[:, LANES:]


def product(high_ref, low_ref, value):
    high, low = split(value)
    both = dot(high_ref[...], jnp.concatenate([high, low], axis=1))
    return both[:, :LANES] + both[:, LANES:] + dot(low_ref[...], high)


def host_of(row, col):
    band, pair, lower = row // 8, (row % 8) // 2, row % 2
    ring = band + (band // 2) * (3 - 2 * band)
    placed = ring + ((lower + pair) % 2) * (3 - 2 * ring)
    level = pair + ring * (3 - 2 * pair)
    return 8 * placed + 2 * level + col % 2, 2 * (col // 2) + band // 2


def tile_of(ty, tx):
    placed, level = ty // 8, (ty % 8) // 2
    ring = placed + (placed // 2) * (3 - 2 * placed)
    pair = level + ring * (3 - 2 * level)
    band = ring + (tx % 2) * (3 - 2 * ring)
    lower = (placed // 2 + pair) % 2
    return 8 * band + 2 * pair + lower, 2 * (tx // 2) + ty % 2


def across(ty, tx):
    return 8 * (3 - ty // 8) + ty % 8, tx


def steps_of(ty, tx):
    to_ty, to_tx = host_of(ty, tx)
    turns = to_ty // 8 != ty // 8
    climbs = ((to_ty % 8) // 2 != (ty % 8) // 2) | (to_tx % 2 != tx % 2)
    return turns & climbs


def kernel(
    n_ty, n_tx, ctrl, iwt, cwt, icols, ccols, marks, out,
    field, iw, cw, ic, cc, mk, relay_field, relay_iw, relay_cw, relay_ic, relay_cc, relay_mk,
    sends, recvs, owned, dense, dense_t, pick, spread, results,
    first_sem, home_sem, relay_sem, pass_sem, send_sem, recv_sem, back_sem, done_sem,
):
    ty, tx = lax.axis_index("ty"), lax.axis_index("tx")
    own_rows = pick.shape[1]
    slots = pick.shape[0]
    extent = own_rows + slots
    slot = slots // 8
    chunks = recvs.shape[1]
    grid_rows = ctrl.shape[0]
    blocks = iw.shape[0]

    row, col = tile_of(ty, tx)
    host = host_of(ty, tx)
    partner = across(ty, tx)
    relayed = host_of(*partner)
    feeder = across(row, col)

    stays = (host[0] == ty) & (host[1] == tx)
    by_relay = steps_of(ty, tx)
    direct = jnp.logical_not(stays | by_relay)
    relays = steps_of(*partner)

    def device(slot_id, sign):
        row_off, col_off = DIRECTIONS[slot_id]
        return host_of(
            (row + sign * row_off + n_ty) % n_ty, (col + sign * col_off + n_tx) % n_tx
        )

    barrier = pltpu.get_barrier_semaphore()
    greeted = [device(slot_id, FORWARD) for slot_id in range(8)]
    greeted += [host, (row, col), partner, feeder]
    for other in greeted:
        pl.semaphore_signal(barrier, inc=1, device_id=other, device_id_type=MESH)
    pl.semaphore_wait(barrier, len(greeted))

    def lanes_of(chunk):
        return pl.ds(chunk * LANES, LANES)

    mine = [icols, ccols, marks] + [iwt.at[b] for b in range(blocks)] + [cwt.at[b] for b in range(blocks)]
    mine += [ctrl.at[:, lanes_of(c)] for c in range(chunks)]
    final = [ic, cc, mk] + [iw.at[b] for b in range(blocks)] + [cw.at[b] for b in range(blocks)]
    final += [field.at[c] for c in range(chunks)]
    passing = [relay_ic, relay_cc, relay_mk] + [relay_iw.at[b] for b in range(blocks)]
    passing += [relay_cw.at[b] for b in range(blocks)]
    passing += [relay_field.at[c] for c in range(chunks)]
    items = len(mine)
    order = [0, 1, 2, 3, 4, 5, 6, 11, 7, 8, 9, 10, 12, 13, 14, 15]

    def to_host(item):
        return pltpu.make_async_remote_copy(
            src_ref=mine[item], dst_ref=final[item],
            send_sem=first_sem.at[item], recv_sem=home_sem.at[item],
            device_id=host, device_id_type=MESH,
        )

    def to_relay(item):
        return pltpu.make_async_remote_copy(
            src_ref=mine[item], dst_ref=passing[item],
            send_sem=first_sem.at[item], recv_sem=relay_sem.at[item],
            device_id=partner, device_id_type=MESH,
        )

    def pass_on(item):
        return pltpu.make_async_remote_copy(
            src_ref=passing[item], dst_ref=final[item],
            send_sem=pass_sem.at[item], recv_sem=home_sem.at[item],
            device_id=relayed, device_id_type=MESH,
        )

    @pl.when(by_relay)
    def _():
        for item in order:
            to_relay(item).start()

    @pl.when(direct)
    def _():
        for item in order:
            to_host(item).start()

    @pl.when(stays)
    def _():
        for item in range(items):
            pltpu.make_async_copy(mine[item], final[item], home_sem.at[item]).start()

    @pl.when(relays)
    def _():
        for item in order:
            to_relay(item).wait_recv()
            pass_on(item).start()

    def landed(item):
        to_host(item).wait_recv()

    def densify(which, weights, cols):
        def step(block, _):
            rows = lax.broadcasted_iota(jnp.int32, (extent, weights.shape[2]), 0)
            onehot = jnp.where(rows == cols[pl.ds(block, 1), :], 1.0, 0.0).astype(jnp.bfloat16)
            high, low = split(weights[block])
            lanes = pl.ds(pl.multiple_of(block * LANES, LANES), LANES)
            turned = dot_rows(onehot, high) + dot_rows(onehot, low)
            plain = dot_rows(high, onehot) + dot_rows(low, onehot)
            high, low = split(turned)
            dense_t[which, 0, :, lanes] = high
            dense_t[which, 1, :, lanes] = low
            high, low = split(plain)
            dense[which, 0, lanes, :] = high
            dense[which, 1, lanes, :] = low
            return 0

        lax.fori_loop(0, blocks, step, 0)

    def copy(stage, chunk, slot_id, sign):
        rows = pl.ds(slot_id * slot, slot)
        return pltpu.make_async_remote_copy(
            src_ref=sends.at[stage, chunk, rows],
            dst_ref=recvs.at[stage, chunk, rows],
            send_sem=send_sem.at[stage, chunk],
            recv_sem=recv_sem.at[stage, chunk],
            device_id=device(slot_id, sign),
            device_id_type=MESH,
        )

    def send(stage, chunk, sign):
        for slot_id in (1, 6, 0, 2, 5, 7, 3, 4):
            copy(stage, chunk, slot_id, sign).start()

    def whole(stage, chunk):
        return pltpu.make_async_remote_copy(
            src_ref=sends.at[stage, chunk],
            dst_ref=recvs.at[stage, chunk],
            send_sem=send_sem.at[stage, chunk],
            recv_sem=recv_sem.at[stage, chunk],
            device_id=device(0, FORWARD),
            device_id_type=MESH,
        )

    slot_rows = lax.broadcasted_iota(jnp.int32, (slots, LANES), 0)
    first, last = row == 0, row == n_ty - 1

    def arrived(stage, chunk, sign):
        whole(stage, chunk).wait_recv()
        top, bottom = (first, last) if sign == ADJOINT else (last, first)
        missing = ((slot_rows < 3 * slot) & top) | ((slot_rows >= 5 * slot) & bottom)
        return jnp.where(missing, 0.0, recvs[stage, chunk])

    heads = items - 2 * blocks - chunks
    for item in range(heads + blocks):
        landed(item)
    grid_ids = lax.broadcasted_iota(jnp.int32, (grid_rows, LANES), 0)

    def inside():
        return grid_ids < mk[0:1, slot : slot + 1]

    densify(0, iw, ic)
    rows = lax.broadcasted_iota(jnp.int32, (own_rows, slot), 0)
    for piece in range(slots // LANES):
        pair = [mk[pl.ds(2 * piece + k, 1), 0:slot] for k in range(2)]
        hot = jnp.concatenate([jnp.where(rows == k, 1.0, 0.0) for k in pair], axis=1)
        lanes = pl.ds(piece * LANES, LANES)
        spread[:, lanes] = hot.astype(jnp.bfloat16)
        pick[lanes, :] = hot.T.astype(jnp.bfloat16)
    for item in range(heads + blocks, heads + 2 * blocks):
        landed(item)
    densify(1, cw, cc)

    def field_landed(chunk):
        pltpu.make_async_remote_copy(
            src_ref=results.at[chunk], dst_ref=field.at[chunk],
            send_sem=first_sem.at[heads + 2 * blocks + chunk],
            recv_sem=home_sem.at[heads + 2 * blocks + chunk],
            device_id=host, device_id_type=MESH,
        ).wait_recv()

    def stage0(chunk):
        field_landed(chunk)
        masked = jnp.where(inside(), field[chunk], 0.0)
        ext = product(dense_t.at[0, 0], dense_t.at[0, 1], masked)
        owned[chunk] = ext[:own_rows]
        sends[0, chunk] = ext[own_rows:]
        send(0, chunk, ADJOINT)

    def stage1(chunk):
        total = owned[chunk] + select(spread[...], arrived(0, chunk, ADJOINT))
        ext = product(dense_t.at[1, 0], dense_t.at[1, 1], total)
        owned[chunk] = ext[:own_rows]
        sends[1, chunk] = ext[own_rows:]
        send(1, chunk, ADJOINT)

    def stage2(chunk):
        total = owned[chunk] + select(spread[...], arrived(1, chunk, ADJOINT))
        owned[chunk] = total
        sends[2, chunk] = select(pick[...], total)
        send(2, chunk, FORWARD)

    def stage3(chunk):
        ext = jnp.concatenate([owned[chunk], arrived(2, chunk, FORWARD)], axis=0)
        smooth = product(dense.at[1, 0], dense.at[1, 1], ext)
        owned[chunk] = smooth
        sends[3, chunk] = select(pick[...], smooth)
        send(3, chunk, FORWARD)

    def back(chunk):
        lanes = pl.ds(pl.multiple_of(chunk * LANES, LANES), LANES)
        return pltpu.make_async_remote_copy(
            src_ref=results.at[chunk], dst_ref=out.at[:, lanes],
            send_sem=back_sem.at[chunk], recv_sem=done_sem.at[chunk],
            device_id=(row, col), device_id_type=MESH,
        )

    def stage4(chunk):
        ext = jnp.concatenate([owned[chunk], arrived(3, chunk, FORWARD)], axis=0)
        result = product(dense.at[0, 0], dense.at[0, 1], ext)
        results[chunk] = jnp.where(inside(), result, 0.0)

        @pl.when(stays)
        def _():
            lanes = pl.ds(pl.multiple_of(chunk * LANES, LANES), LANES)
            pltpu.make_async_copy(results.at[chunk], out.at[:, lanes], done_sem.at[chunk]).start()

        @pl.when(jnp.logical_not(stays))
        def _():
            back(chunk).start()

    stages = (stage0, stage1, stage2, stage3, stage4)

    def run(stage):
        def one(chunk, _):
            stage(chunk)
            return 0

        lax.fori_loop(0, chunks, one, 0)

    for stage in stages:
        run(stage)

    @pl.when(by_relay | direct)
    def _():
        for item in range(items):
            to_host(item).wait_send()

    @pl.when(relays)
    def _():
        for item in range(items):
            pass_on(item).wait_send()

    @pl.when(jnp.logical_not(stays))
    def _():
        for chunk in range(chunks):
            back(chunk).wait_send()

    for chunk in range(chunks):
        for stage in range(4):
            whole(stage, chunk).wait_send()
        back(chunk).wait_recv()


def body(n_ty, n_tx, ctrl, interp_wt, interp_cols, conv_wt, conv_cols, halo_index, valid):
    field = ctrl[0, 0]
    iwt, cwt = interp_wt[0, 0], conv_wt[0, 0]
    grid_rows, width = field.shape
    blocks = iwt.shape[0]
    own_rows = blocks * cwt.shape[1]
    slots = halo_index.shape[2] * halo_index.shape[3]
    extent = own_rows + slots
    chunks = width // LANES
    halo = halo_index[0, 0]
    marks = jnp.concatenate([halo, jnp.broadcast_to(valid, halo.shape)], axis=1)
    icols, ccols = interp_cols[0, 0], conv_cols[0, 0]
    hbm = pl.BlockSpec(memory_space=pl.ANY)
    f32, bf16 = jnp.float32, jnp.bfloat16
    tile = [
        pltpu.VMEM((chunks, grid_rows, LANES), f32),
        pltpu.VMEM(iwt.shape, f32),
        pltpu.VMEM(cwt.shape, f32),
        pltpu.VMEM(icols.shape, jnp.int32),
        pltpu.VMEM(ccols.shape, jnp.int32),
        pltpu.VMEM(marks.shape, jnp.int32),
    ]
    items = 3 + 2 * blocks + chunks
    dma = pltpu.SemaphoreType.DMA
    result = pl.pallas_call(
        functools.partial(kernel, n_ty, n_tx),
        out_shape=jax.ShapeDtypeStruct((grid_rows, width), f32),
        in_specs=[hbm] * 6,
        out_specs=hbm,
        scratch_shapes=tile
        + tile
        + [
            pltpu.VMEM((4, chunks, slots, LANES), f32),
            pltpu.VMEM((4, chunks, slots, LANES), f32),
            pltpu.VMEM((chunks, own_rows, LANES), f32),
            pltpu.VMEM((2, 2, own_rows, extent), bf16),
            pltpu.VMEM((2, 2, extent, own_rows), bf16),
            pltpu.VMEM((slots, own_rows), bf16),
            pltpu.VMEM((own_rows, slots), bf16),
            pltpu.VMEM((chunks, grid_rows, LANES), f32),
            dma((items,)),
            dma((items,)),
            dma((items,)),
            dma((items,)),
            dma((4, chunks)),
            dma((4, chunks)),
            dma((chunks,)),
            dma((chunks,)),
        ],
        compiler_params=pltpu.CompilerParams(collective_id=0, has_side_effects=True),
    )(field, iwt, cwt, icols, ccols, marks)
    return result[None, None]


def solution(mesh):
    placed = (
        P("ty", "tx", None, None),
        P("ty", "tx", None, None, None),
        P("ty", "tx", None, None),
        P("ty", "tx", None, None, None),
        P("ty", "tx", None, None),
        P("ty", "tx", None, None),
        P("ty", "tx"),
    )
    return jax.shard_map(
        functools.partial(body, mesh.shape["ty"], mesh.shape["tx"]),
        mesh=mesh,
        in_specs=placed,
        out_specs=P("ty", "tx", None, None),
        check_vma=False,
    )
```
